128 devices in a mesh: section: 8 (over y_hi, x), seq: 16 (over z, y_lo, core).
Axes of the slice: x: 4, y: 4 (y_hi: 2, y_lo: 2; y = y_hi * 2 + y_lo), z: 4, core: 2. Of those that a mesh axis runs over, the one named last changes fastest.
Arguments:
- tokens: bfloat16 [8, 4096, 4096], P('section', 'seq'), may hold values from -6 to 6
- norm_gain: bfloat16 [8, 4096], P('section'), may hold values from 0.099609375 to 1.8984375
- w_query: bfloat16 [8, 4096, 2048], P('section', 'seq'), may hold values from -0.09375 to 0.09375
- w_key: bfloat16 [8, 4096, 512], P('section', 'seq'), may hold values from -1.903125 to 1.903125
- w_value: bfloat16 [8, 4096, 512], P('section', 'seq'), may hold values from -0.09375 to 0.09375
Outputs:
- received: bfloat16 [8, 4096, 2048], P('section', 'seq')
The draws below stay inside these ranges and needn't reach their ends.
All inputs are finite; a program needn't handle non-finite values.
Results may differ from the reference program's by a relative error of at most 0.012.
The reference program's roundings to bfloat16 on the way count: a program that leaves them out, or rounds other values in their place, can miss the bound.
Values may be sent and summed in bfloat16 or wider, within the bound.
No kernel may reach another device: no remote copies, remote signals or barrier semaphores. Data moves between devices by JAX's collectives and lax.ppermute only.
A program may use at most 192 MiB of HBM per device.

```python
import jax
import jax.numpy as jnp
from jax import lax

MODEL_WIDTH = 4096
LOCAL_QUERY_HEADS = 16
LOCAL_KEY_HEADS = 4
HEAD_SIZE = 128
SECTION_COUNT = 8
TOKENS = 4096
KW = 512


def paired_weights(key):
    query_portion = jax.random.normal(jax.random.fold_in(key, 101), (SECTION_COUNT, MODEL_WIDTH, LOCAL_QUERY_HEADS * HEAD_SIZE), jnp.float32)
    query_portion = jnp.clip(query_portion, -6.0, 6.0) * MODEL_WIDTH ** (-0.5)
    key_portion = jnp.clip(jax.random.normal(jax.random.fold_in(key, 104), (SECTION_COUNT, MODEL_WIDTH, LOCAL_KEY_HEADS * HEAD_SIZE), jnp.float32), -6.0, 6.0) * MODEL_WIDTH ** (-0.5)
    return (query_portion, key_portion)


def draw_w_query(key, part):
    return paired_weights(key)[0].astype(jnp.bfloat16)


def draw_w_key(key, part):
    return paired_weights(key)[1].astype(jnp.bfloat16)


def block_levels(key, extent, shards, low, top_value):
    def one(position, parts):
        heights = jax.random.uniform(jax.random.fold_in(jax.random.fold_in(key, 6), position), (parts,), jnp.float32, low / len(shards), top_value / len(shards))
        return jnp.repeat(jnp.exp(heights), extent[position] // parts).reshape((-1,) + (1,) * (len(extent) - position - 1))

    loudness = one(*shards[0])
    for cut in shards[1:]:
        loudness = loudness * one(*cut)
    return loudness


def centred(stream_key, shape, scale, limit, shards=(), dtype=jnp.bfloat16):
    values = jax.random.normal(stream_key, shape, jnp.float32) * scale
    if len(shards) > 0:
        values = block_levels(stream_key, shape, shards, -0.22, 0.18) * values
    return jnp.clip(values, min=-limit, max=limit).astype(dtype)


def setup_inputs(seed: int = 0) -> dict:
    keys = jax.random.split(jax.random.key(seed), 6)
    return {
        "tokens": centred(keys[0], (SECTION_COUNT, TOKENS, MODEL_WIDTH), 1.0, 6.0, ((0, 8), (1, 16))),
        "norm_gain": jnp.clip(1.0 + 0.18 * jax.random.normal(keys[1], (SECTION_COUNT, MODEL_WIDTH), jnp.float32), 0.099609375, 1.8984375).astype(jnp.bfloat16),
        "w_query": draw_w_query(jax.random.fold_in(keys[5], 71), 0),
        "w_key": draw_w_key(jax.random.fold_in(keys[5], 71), 0),
        "w_value": centred(keys[4], (SECTION_COUNT, MODEL_WIDTH, KW), MODEL_WIDTH ** -0.5, 0.09375, ((0, 8), (1, 16))),
    }


def normalize(rows_in, gain_row):
    wide = rows_in.astype(jnp.float32)
    scale = lax.rsqrt(lax.optimization_barrier(jnp.mean(wide * wide, axis=-1, keepdims=True)) + 1e-05)
    return (wide * scale * gain_row.astype(jnp.float32)).astype(jnp.bfloat16)

def rotate(matrix, positions):
    row_count = matrix.shape[0]
    head_count = matrix.shape[1] // HEAD_SIZE
    half_dim = HEAD_SIZE // 2
    shaped = matrix.reshape(row_count, head_count, HEAD_SIZE)
    freqs = jnp.power(jnp.float32(500000.0), -(jnp.arange(half_dim).astype(jnp.float32) * 2.0 / HEAD_SIZE))
    angles = positions[:, None] * freqs[None, :]
    cosine = jnp.cos(angles)[:, None, :]
    sine_part = jnp.sin(angles)[:, None, :]
    first_half = shaped[:, :, :half_dim]
    second_half = shaped[:, :, half_dim:]
    turned = jnp.concatenate([first_half * cosine - second_half * sine_part, second_half * cosine + first_half * sine_part], axis=2)
    return turned.reshape(row_count, head_count * HEAD_SIZE)

def expand(matrix):
    row_count = matrix.shape[0]
    kv_count = matrix.shape[1] // HEAD_SIZE
    query_group_count = LOCAL_QUERY_HEADS // LOCAL_KEY_HEADS
    wide = jnp.broadcast_to(matrix.reshape(row_count, kv_count, 1, HEAD_SIZE), (row_count, kv_count, query_group_count, HEAD_SIZE))
    return wide.reshape(row_count, kv_count * query_group_count * HEAD_SIZE)

def attend(queries, key_rows, value_rows):
    row_count = queries.shape[0]
    head_count = queries.shape[1] // HEAD_SIZE
    block_rows = min(512, row_count)
    key_heads = key_rows.reshape(row_count, head_count, HEAD_SIZE).astype(jnp.float32)
    value_heads = value_rows.reshape(row_count, head_count, HEAD_SIZE).astype(jnp.float32)
    key_places = jnp.arange(row_count).astype(jnp.int32)

    def one_block(block_index):
        first_row = (block_index * block_rows).astype(jnp.int32)
        query_block = lax.dynamic_slice_in_dim(queries, first_row, block_rows, 0)
        query_block = query_block.reshape(block_rows, head_count, HEAD_SIZE).astype(jnp.float32)
        scores = jnp.einsum('qhd,khd->hqk', query_block, key_heads, precision=lax.Precision.HIGHEST) / jnp.sqrt(jnp.float32(HEAD_SIZE))
        query_places = first_row + jnp.arange(block_rows).astype(jnp.int32)
        causal = key_places[None, :] <= query_places[:, None]
        scores = jnp.where(causal[None, :, :], scores, -jnp.inf)
        maxima = lax.optimization_barrier(jnp.max(scores, axis=-1, keepdims=True))
        expon = jnp.exp(scores - maxima)
        probs = (expon / lax.optimization_barrier(jnp.sum(expon, axis=-1, keepdims=True))).astype(jnp.bfloat16)
        mixed = jnp.einsum('hqk,khd->qhd', probs.astype(jnp.float32), value_heads, precision=lax.Precision.HIGHEST)
        return mixed.astype(jnp.bfloat16).reshape(block_rows, head_count * HEAD_SIZE)
    blocks = lax.map(one_block, jnp.arange(row_count // block_rows).astype(jnp.int32))
    return blocks.reshape(row_count, head_count * HEAD_SIZE)

def layer(operands):
    section_tokens, gain_row, query_weight, key_weight, value_weight = operands
    normed = normalize(section_tokens, gain_row)
    positions = jnp.arange(normed.shape[0]).astype(jnp.float32)
    queries = rotate(jnp.dot(normed, query_weight, preferred_element_type=jnp.float32), positions).astype(jnp.bfloat16)
    key_rows = rotate(jnp.dot(normed, key_weight, preferred_element_type=jnp.float32), positions).astype(jnp.bfloat16)
    value_rows = jnp.dot(normed, value_weight, preferred_element_type=jnp.float32).astype(jnp.bfloat16)
    return attend(queries, expand(key_rows), expand(value_rows))

def reference(tokens, norm_gain, w_query, w_key, w_value):
    outputs = lax.map(layer, (tokens, norm_gain, w_query, w_key, w_value))
    return jnp.roll(outputs, 1, axis=0)
```

```python
import math

import jax
import jax.numpy as jnp
from jax import lax
from jax.experimental import pallas as pl
from jax.experimental.pallas import tpu as pltpu
from jax.sharding import PartitionSpec as P

HEAD = 128
GROUP = 4
RING = 4
LOG2E_SCALE = math.log2(math.e) / math.sqrt(HEAD)
NEG = -1e30


def near(block, bits):
    return lax.ppermute(block, "seq", [(r, r ^ bits) for r in range(RING * GROUP)])


def along(block, step):
    n = RING * GROUP
    return lax.ppermute(block, "seq", [(r, (r + step * GROUP) % n) for r in range(n)])


def onward(block, bits):
    n = RING * GROUP
    s = lax.axis_size("section")
    route = [(i * n + r, ((i + 1) % s) * n + (r ^ bits)) for i in range(s) for r in range(n)]
    return lax.ppermute(block, ("section", "seq"), route)


def normalize(rows_in, gain_row):
    wide = rows_in.astype(jnp.float32)
    scale = lax.rsqrt(jnp.mean(wide * wide, axis=-1, keepdims=True) + 1e-05)
    return (wide * scale * gain_row.astype(jnp.float32)).astype(jnp.bfloat16)


def rope_tables(rank, z, g, rows):
    blocks = jnp.stack([z * GROUP + (g ^ j) for j in range(GROUP)])
    positions = (blocks[:, None] * rows + jnp.arange(rows)[None, :]).reshape(-1).astype(jnp.float32)
    half = HEAD // 2
    freqs = jnp.power(jnp.float32(500000.0), -(jnp.arange(half).astype(jnp.float32) * 2.0 / HEAD))
    angles = positions[:, None] * freqs[None, :]
    cosine, sine = jnp.cos(angles), jnp.sin(angles)
    return jnp.concatenate([cosine, cosine], axis=1), jnp.concatenate([-sine, sine], axis=1)


def project(place, tokens, weights, cos_table, sin_table):
    rows = sum(t.shape[0] for t in tokens)
    width = tokens[0].shape[1]
    depth = weights[0][0].shape[0]
    n_tok = len(tokens)
    flat = [w for slab in weights for w in slab]
    tile = 2 * HEAD

    def kernel(place_ref, *refs):
        tok = refs[:n_tok]
        wts = refs[n_tok : n_tok + len(flat)]
        cos_ref, sin_ref, q_ref, kv_ref = refs[n_tok + len(flat) :]
        step = pl.program_id(0)
        z, g = place_ref[0], place_ref[1]
        starts = []
        for off in range(RING):
            for j in range(GROUP):
                starts.append(pl.multiple_of((((z + off) % RING) * GROUP + (g ^ j)) * depth, depth))
        base = 0
        for t in tok:
            n = t.shape[0]
            raw = None
            for start, w in zip(starts, wts):
                part = jnp.dot(t[:, pl.ds(start, depth)], w[...], preferred_element_type=jnp.float32)
                raw = part if raw is None else raw + part
            c = cos_ref[pl.ds(base, n), :]
            s = sin_ref[pl.ds(base, n), :]
            first, second = raw[:, :HEAD], raw[:, HEAD:]
            first_turned = first * c + pltpu.roll(first, HEAD // 2, 1) * s

            def put_q(base=base, n=n, second=second, first_turned=first_turned, c=c, s=s):
                second_turned = second * c + pltpu.roll(second, HEAD // 2, 1) * s
                q_ref[pl.ds(base, n), :HEAD] = first_turned.astype(jnp.bfloat16)
                q_ref[pl.ds(base, n), HEAD:] = second_turned.astype(jnp.bfloat16)

            def put_kv(base=base, n=n, second=second, first_turned=first_turned):
                kv_ref[pl.ds(base, n), :HEAD] = first_turned.astype(jnp.bfloat16)
                kv_ref[pl.ds(base, n), HEAD:] = second.astype(jnp.bfloat16)

            pl.when(step < 2)(put_q)
            pl.when(step == 2)(put_kv)
            base += n

    fixed = lambda n, place: (0, 0)
    return pl.pallas_call(
        kernel,
        grid_spec=pltpu.PrefetchScalarGridSpec(
            num_scalar_prefetch=1,
            grid=(3,),
            in_specs=[pl.BlockSpec(t.shape, fixed) for t in tokens]
            + [pl.BlockSpec((depth, tile), lambda n, place: (0, n)) for _ in flat]
            + [pl.BlockSpec((rows, HEAD), fixed)] * 2,
            out_specs=[
                pl.BlockSpec((rows, tile), lambda n, place: (0, jnp.minimum(n, 1))),
                pl.BlockSpec((rows, tile), fixed),
            ],
        ),
        out_shape=[
            jax.ShapeDtypeStruct((rows, 2 * tile), jnp.bfloat16),
            jax.ShapeDtypeStruct((rows, tile), jnp.bfloat16),
        ],
        compiler_params=pltpu.CompilerParams(vmem_limit_bytes=48 << 20),
        cost_estimate=pl.CostEstimate(
            flops=2 * rows * width * 3 * tile, transcendentals=0, bytes_accessed=2 * (rows * width + width * 3 * tile)
        ),
    )(place, *tokens, *flat, cos_table, sin_table)


def attend(place, queries, own, below, order, block):
    rows = 256
    heads = GROUP
    flat = list(own) + [p for slab in below for p in slab]

    def kernel(place_ref, q_ref, *refs):
        kv = refs[: len(flat)]
        out_ref, acc_ref, top_ref = refs[len(flat) :]
        z, g = place_ref[0], place_ref[1]
        mine = g ^ order

        def visit(pieces, masked, first):
            keys = [p[:, :HEAD] for p in pieces]
            k = keys[0] if len(keys) == 1 else jnp.concatenate(keys, axis=0)
            values = [p[:, HEAD:] for p in pieces]
            v = values[0] if len(values) == 1 else jnp.concatenate(values, axis=0)
            v = jnp.concatenate([v, jnp.ones_like(v)], axis=1)
            for h in range(heads):
                q = q_ref[:, h * HEAD : (h + 1) * HEAD]
                s = lax.dot_general(q, k, (((1,), (1,)), ((), ())), preferred_element_type=jnp.float32)
                if masked:
                    at = lax.broadcasted_iota(jnp.int32, s.shape, 0)
                    key_at = lax.broadcasted_iota(jnp.int32, s.shape, 1)
                    s = jnp.where(key_at <= at, s, NEG)
                top = jnp.max(s, axis=1, keepdims=True)
                if not first:
                    old = top_ref[h][:, :1]
                    top = jnp.maximum(top, old)
                p = jnp.exp2((s - top) * LOG2E_SCALE).astype(jnp.bfloat16)
                new = jnp.dot(p, v, preferred_element_type=jnp.float32)
                if not first:
                    new = new + acc_ref[h] * jnp.exp2((old - top) * LOG2E_SCALE)
                acc_ref[h] = new
                top_ref[h] = jnp.broadcast_to(top, (rows, HEAD))

        def window(ref, start):
            return ref.at[pl.ds(start, 256), :]

        pieces = []
        for ref in kv[: len(own)]:
            for start in range(0, ref.shape[0], 256):
                pieces.append(window(ref, start))
        visit([pieces[order]], True, True)
        for j in range(GROUP):
            if j != order:
                pl.when((g ^ j) < mine)(lambda j=j: visit([pieces[j]], False, False))
        at = len(own)
        for d, slab in enumerate(below, start=1):
            refs_d = kv[at : at + len(slab)]
            at += len(slab)
            pl.when(z >= d)(lambda refs_d=refs_d: visit(list(refs_d), False, False))
        for h in range(heads):
            total = acc_ref[h]
            out_ref[:, h * HEAD : (h + 1) * HEAD] = (total[:, :HEAD] / total[:, HEAD:]).astype(jnp.bfloat16)

    whole = lambda i, place: (0, 0)
    return pl.pallas_call(
        kernel,
        grid_spec=pltpu.PrefetchScalarGridSpec(
            num_scalar_prefetch=1,
            grid=(1,),
            in_specs=[pl.BlockSpec((rows, heads * HEAD), lambda i, place: (block, 0))]
            + [pl.BlockSpec(p.shape, whole) for p in flat],
            out_specs=pl.BlockSpec((rows, heads * HEAD), whole),
            scratch_shapes=[
                pltpu.VMEM((heads, rows, 2 * HEAD), jnp.float32),
                pltpu.VMEM((heads, rows, HEAD), jnp.float32),
            ],
        ),
        out_shape=jax.ShapeDtypeStruct((rows, heads * HEAD), jnp.bfloat16),
        compiler_params=pltpu.CompilerParams(vmem_limit_bytes=48 << 20),
        cost_estimate=pl.CostEstimate(
            flops=4 * rows * heads * HEAD * 4096, transcendentals=rows * heads * 4096, bytes_accessed=3 << 20
        ),
    )(place, queries, *flat)


def per_device(tokens, norm_gain, w_query, w_key, w_value):
    rank = lax.axis_index("seq")
    z, g = rank // GROUP, rank % GROUP
    place = jnp.stack([z, g]).astype(jnp.int32)
    rows = tokens.shape[1]

    def columns(j):
        c = g ^ j
        take = lambda w, n: lax.dynamic_slice_in_dim(w[0], c * n, n, 1)
        return jnp.concatenate([take(w_query, 4 * HEAD), take(w_key, HEAD), take(w_value, HEAD)], axis=1)

    here = [columns(0)]
    here += [near(columns(j), j) for j in (1, 2, 3)]
    left = [along(w, 1) for w in here]
    right = [along(w, -1) for w in here]
    far = [along(left[0], 1), along(left[1], 1), along(right[2], -1), along(right[3], -1)]
    weights = [here, right, far, left]

    normed = normalize(tokens[0], norm_gain[0])
    side = near(normed, 1)
    half = rows // 2
    across = [near(normed[i * half : (i + 1) * half], 2) for i in range(2)]
    corner = [near(a, 1) for a in across]

    cos_table, sin_table = rope_tables(rank, z, g, rows)
    q_a, kv_a = project(place, [normed, side], weights, cos_table[: 2 * rows], sin_table[: 2 * rows])
    q_b, kv_b = project(place, across + corner, weights, cos_table[2 * rows :], sin_table[2 * rows :])

    below = [[], [], []]
    for kv in (kv_a, kv_b):
        from_left = along(kv, 1)
        from_right = along(kv, -1)
        below[0].append(from_left)
        below[2].append(from_right)
        below[1].append(along(from_left[:rows], 1))
        below[1].append(along(from_right[rows:], -1))

    out = jnp.zeros((rows, GROUP * GROUP * HEAD), jnp.bfloat16)
    for k in range(GROUP):
        mixed = attend(place, q_a if k < 2 else q_b, [kv_a, kv_b], below, k, k % 2)
        arrived = onward(mixed, k)
        out = lax.dynamic_update_slice(out, arrived, (0, (g ^ k) * GROUP * HEAD))
    return out[None]


def solution(mesh):
    return jax.shard_map(
        per_device,
        mesh=mesh,
        in_specs=(
            P("section", "seq", None),
            P("section", None),
            P("section", "seq", None),
            P("section", "seq", None),
            P("section", "seq", None),
        ),
        out_specs=P("section", "seq", None),
        check_vma=False,
    )
```

```python
import math

import jax
import jax.numpy as jnp
from jax import lax
from jax.experimental import pallas as pl
from jax.experimental.pallas import tpu as pltpu
from jax.sharding import PartitionSpec as P


HEAD = 128
GROUP = 4
RING = 4
LOG2E_SCALE = math.log2(math.e) / math.sqrt(HEAD)
NEG = -1e30


def near(block, bits):
    return lax.ppermute(block, "seq", [(r, r ^ bits) for r in range(RING * GROUP)])


def along(block, step):
    n = RING * GROUP
    return lax.ppermute(block, "seq", [(r, (r + step * GROUP) % n) for r in range(n)])


def onward(block, bits):
    n = RING * GROUP
    s = lax.axis_size("section")
    route = [(i * n + r, ((i + 1) % s) * n + (r ^ bits)) for i in range(s) for r in range(n)]
    return lax.ppermute(block, ("section", "seq"), route)


def normalize(rows_in, gain_row):
    wide = rows_in.astype(jnp.float32)
    scale = lax.rsqrt(jnp.mean(wide * wide, axis=-1, keepdims=True) + 1e-05)
    return (wide * scale * gain_row.astype(jnp.float32)).astype(jnp.bfloat16)


def rope_tables(z, g, rows):
    blocks = jnp.stack([z * GROUP + (g ^ j) for j in range(GROUP)])
    positions = (blocks[:, None] * rows + jnp.arange(rows)[None, :]).reshape(-1).astype(jnp.float32)
    half = HEAD // 2
    freqs = jnp.power(jnp.float32(500000.0), -(jnp.arange(half).astype(jnp.float32) * 2.0 / HEAD))
    angles = positions[:, None] * freqs[None, :]
    cosine, sine = jnp.cos(angles), jnp.sin(angles)
    return jnp.concatenate([cosine, cosine], axis=1), jnp.concatenate([-sine, sine], axis=1)


def project(place, tokens, weights, cos_table, sin_table):
    rows = sum(t.shape[0] for t in tokens)
    width = tokens[0].shape[1]
    n_tok = len(tokens)
    depth = width // (RING * GROUP)
    flat = [w for slab in weights for w in slab]
    tile = 2 * HEAD

    def kernel(place_ref, *refs):
        tok = refs[:n_tok]
        wts = refs[n_tok : n_tok + len(flat)]
        cos_ref, sin_ref, q_ref, kv_ref = refs[n_tok + len(flat) :]
        z, g = place_ref[0], place_ref[1]
        blocks = []
        at = 0
        for off in range(RING):
            j = 0
            for w in weights[off]:
                for row in range(0, w.shape[0], depth):
                    start = pl.multiple_of((((z + off) % RING) * GROUP + (g ^ j)) * depth, depth)
                    blocks.append((start, wts[at], row))
                    j += 1
                at += 1
        c, s = cos_ref[...], sin_ref[...]
        for n in range(3):
            raw = None
            for start, w, row in blocks:
                lhs = [t[:, pl.ds(start, depth)] for t in tok]
                lhs = lhs[0] if n_tok == 1 else jnp.concatenate(lhs, axis=0)
                part = jnp.dot(lhs, w[row : row + depth, n * tile : (n + 1) * tile], preferred_element_type=jnp.float32)
                raw = part if raw is None else raw + part
            first, second = raw[:, :HEAD], raw[:, HEAD:]
            first = first * c + pltpu.roll(first, HEAD // 2, 1) * s
            out, col = (q_ref, n * tile) if n < 2 else (kv_ref, 0)
            if n < 2:
                second = second * c + pltpu.roll(second, HEAD // 2, 1) * s
            out[:, col : col + HEAD] = first.astype(jnp.bfloat16)
            out[:, col + HEAD : col + tile] = second.astype(jnp.bfloat16)

    vmem = pl.BlockSpec(memory_space=pltpu.VMEM)
    return pl.pallas_call(
        kernel,
        in_specs=[pl.BlockSpec(memory_space=pltpu.SMEM)] + [vmem] * (n_tok + len(flat) + 2),
        out_specs=[vmem, vmem],
        out_shape=[
            jax.ShapeDtypeStruct((rows, 2 * tile), jnp.bfloat16),
            jax.ShapeDtypeStruct((rows, tile), jnp.bfloat16),
        ],
        compiler_params=pltpu.CompilerParams(vmem_limit_bytes=40 << 20),
        cost_estimate=pl.CostEstimate(
            flops=2 * rows * width * 3 * tile, transcendentals=0, bytes_accessed=2 * (rows * width + width * 3 * tile)
        ),
    )(place, *tokens, *flat, cos_table, sin_table)


def attend(place, queries, own, below, order, block):
    rows = 256
    heads = GROUP
    flat = list(own) + [p for slab in below for p in slab]
    total = sum(p.shape[0] for p in flat)

    def kernel(place_ref, q_ref, *refs):
        kv = refs[: len(flat)]
        out_ref, s_ref = refs[len(flat) :]
        z, g = place_ref[0], place_ref[1]
        segments = []
        at = 0
        for p in own:
            for _ in range(0, p.shape[0], rows):
                j = at // rows
                segments.append((at, rows, None if j == order else (g ^ j) < (g ^ order)))
                at += rows
        for d, slab in enumerate(below, start=1):
            n = sum(p.shape[0] for p in slab)
            segments.append((at, n, z >= d))
            at += n
        stacked = jnp.concatenate([q_ref[block * rows : (block + 1) * rows, h * HEAD : (h + 1) * HEAD] for h in range(heads)], axis=0)
        at = 0
        for p in kv:
            n = p.shape[0]
            s_ref[:, at : at + n] = lax.dot_general(
                stacked, p[:, :HEAD], (((1,), (1,)), ((), ())), preferred_element_type=jnp.float32
            )
            at += n
        v = jnp.concatenate([p[:, HEAD:] for p in kv], axis=0)
        v = jnp.concatenate([v, jnp.ones_like(v)], axis=1)
        causal = lax.broadcasted_iota(jnp.int32, (rows, rows), 1) <= lax.broadcasted_iota(jnp.int32, (rows, rows), 0)
        for h in range(heads):
            mine = slice(h * rows, (h + 1) * rows)
            scores, top = [], None
            for first, n, visible in segments:
                s = s_ref[mine, first : first + n]
                if visible is None:
                    s = jnp.where(causal, s, NEG)
                scores.append(s)
                best = s[:, :HEAD]
                for lane in range(HEAD, n, HEAD):
                    best = jnp.maximum(best, s[:, lane : lane + HEAD])
                if visible is not None:
                    best = jnp.where(visible, best, NEG)
                top = best if top is None else jnp.maximum(top, best)
            top = jnp.max(top, axis=1, keepdims=True)
            probs = []
            for s, (first, n, visible) in zip(scores, segments):
                less = top if visible is None else jnp.where(visible, top, -NEG)
                probs.append(jnp.exp2((s - less) * LOG2E_SCALE).astype(jnp.bfloat16))
            mixed = jnp.dot(jnp.concatenate(probs, axis=1), v, preferred_element_type=jnp.float32)
            out_ref[:, h * HEAD : (h + 1) * HEAD] = (mixed[:, :HEAD] / mixed[:, HEAD:]).astype(jnp.bfloat16)

    vmem = pl.BlockSpec(memory_space=pltpu.VMEM)
    return pl.pallas_call(
        kernel,
        in_specs=[pl.BlockSpec(memory_space=pltpu.SMEM)] + [vmem] * (1 + len(flat)),
        out_specs=vmem,
        out_shape=jax.ShapeDtypeStruct((rows, heads * HEAD), jnp.bfloat16),
        scratch_shapes=[pltpu.VMEM((heads * rows, total), jnp.float32)],
        compiler_params=pltpu.CompilerParams(vmem_limit_bytes=40 << 20),
        cost_estimate=pl.CostEstimate(
            flops=8 * rows * heads * HEAD * total, transcendentals=rows * heads * total, bytes_accessed=3 << 20
        ),
    )(place, queries, *flat)


def section_tick(tokens, norm_gain, w_query, w_key, w_value):
    rank = lax.axis_index("seq")
    z, g = rank // GROUP, rank % GROUP
    place = jnp.stack([z, g]).astype(jnp.int32)
    rows = tokens.shape[1]
    half = rows // 2

    def columns(j):
        c = g ^ j
        take = lambda w, n: lax.dynamic_slice_in_dim(w[0], c * n, n, 1)
        return jnp.concatenate([take(w_query, 4 * HEAD), take(w_key, HEAD), take(w_value, HEAD)], axis=1)

    got = []
    for j in (1, 2, 3):
        got.append(near(columns(j), j))
    chip = jnp.concatenate([columns(0), got[0]], axis=0)
    other = jnp.concatenate([got[1], got[2]], axis=0)
    chip_left = along(chip, 1)
    chip_right = along(chip, -1)
    other_left = along(other, 1)
    other_right = along(other, -1)
    chip_far = along(chip_left, 1)
    other_far = along(other_right, -1)
    weights = [[chip, other], [chip_right, other_right], [chip_far, other_far], [chip_left, other_left]]

    normed = normalize(tokens[0], norm_gain[0])
    side = near(normed, 1)
    across, corner = [], []
    for i in range(2):
        across.append(near(normed[i * half : (i + 1) * half], 2))
    for i in range(2):
        corner.append(near(across[i], 1))

    cos_table, sin_table = rope_tables(z, g, rows)
    q_a, kv_a = project(place, [normed, side], weights, cos_table[: 2 * rows], sin_table[: 2 * rows])
    q_b, kv_b = project(place, across + corner, weights, cos_table[2 * rows :], sin_table[2 * rows :])

    below = [[], [], []]
    for kv in (kv_a, kv_b):
        from_left = along(kv, 1)
        from_right = along(kv, -1)
        below[0].append(from_left)
        below[2].append(from_right)
        below[1].append(along(from_left[:rows], 1))
        below[1].append(along(from_right[rows:], -1))

    out = jnp.zeros((rows, GROUP * GROUP * HEAD), jnp.bfloat16)
    for k in range(GROUP):
        mixed = attend(place, q_a if k < 2 else q_b, [kv_a, kv_b], below, k, k % 2)
        arrived = onward(mixed, k)
        out = lax.dynamic_update_slice(out, arrived, (0, (g ^ k) * GROUP * HEAD))
    return out[None]


def solution(mesh):
    return jax.shard_map(
        section_tick,
        mesh=mesh,
        in_specs=(
            P("section", "seq", None),
            P("section", None),
            P("section", "seq", None),
            P("section", "seq", None),
            P("section", "seq", None),
        ),
        out_specs=P("section", "seq", None),
        check_vma=False,
    )
```

```python
import math

import jax
import jax.numpy as jnp
from jax import lax
from jax.experimental import pallas as pl
from jax.experimental.pallas import tpu as pltpu
from jax.sharding import PartitionSpec as P


HEAD = 128
GROUP = 4
RING = 4
LOG2E_SCALE = math.log2(math.e) / math.sqrt(HEAD)
NEG = -1e30
PROJECT_VMEM = 10 << 20


def near(block, bits):
    return lax.ppermute(block, "seq", [(r, r ^ bits) for r in range(RING * GROUP)])


def along(block, step):
    n = RING * GROUP
    return lax.ppermute(block, "seq", [(r, (r + step * GROUP) % n) for r in range(n)])


def upward(block, routes):
    return lax.ppermute(block, "seq", [(a * GROUP + g, b * GROUP + g) for a, b in routes for g in range(GROUP)])


def onward(block, bits):
    n = RING * GROUP
    s = lax.axis_size("section")
    route = [(i * n + r, ((i + 1) % s) * n + (r ^ bits)) for i in range(s) for r in range(n)]
    return lax.ppermute(block, ("section", "seq"), route)


def normalize(rows_in, gain_row):
    wide = rows_in.astype(jnp.float32)
    scale = lax.rsqrt(jnp.mean(wide * wide, axis=-1, keepdims=True) + 1e-05)
    return (wide * scale * gain_row.astype(jnp.float32)).astype(jnp.bfloat16)


def rope_tables(z, g, rows, pieces):
    at = [(z * GROUP + (g ^ j)) * rows + first + jnp.arange(n) for j, first, n in pieces]
    positions = jnp.concatenate(at).astype(jnp.float32)
    half = HEAD // 2
    freqs = jnp.power(jnp.float32(500000.0), -(jnp.arange(half).astype(jnp.float32) * 2.0 / HEAD))
    angles = positions[:, None] * jnp.concatenate([freqs, freqs])[None, :]
    sign = jnp.where(jnp.arange(HEAD) < half, -1.0, 1.0).astype(jnp.float32)
    return jnp.cos(angles), jnp.sin(angles) * sign[None, :]


def weight_blocks(place_ref, weights, refs, depth):
    z, g = place_ref[0], place_ref[1]
    blocks, at = [], 0
    for off, slab in enumerate(weights):
        j = 0
        for w in slab:
            for row in range(0, w.shape[0], depth):
                start = pl.multiple_of((((z + off) % RING) * GROUP + (g ^ j)) * depth, depth)
                blocks.append((start, refs[at], row))
                j += 1
            at += 1
    return blocks


def turned(x, c, s):
    return (x * c + pltpu.roll(x, HEAD // 2, 1) * s).astype(jnp.bfloat16)


def project(place, chunks, weights, cos_table, sin_table, queries):
    tokens = [t for chunk in chunks for t in chunk]
    rows = sum(t.shape[0] for t in tokens)
    width = tokens[0].shape[1]
    depth = width // (RING * GROUP)
    flat = [w for slab in weights for w in slab]
    tile = 2 * HEAD
    out_width = 2 * tile if queries else tile

    def kernel(place_ref, *refs):
        tok = refs[: len(tokens)]
        wts = refs[len(tokens) : len(tokens) + len(flat)]
        cos_ref, sin_ref, out_ref = refs[len(tokens) + len(flat) :]
        blocks = weight_blocks(place_ref, weights, wts, depth)

        def columns(first_column, out_column):
            at, base = 0, 0
            for chunk in chunks:
                mine = tok[at : at + len(chunk)]
                at += len(chunk)
                n = sum(t.shape[0] for t in chunk)
                raw = None
                for start, w, row in blocks:
                    lhs = jnp.concatenate([t[:, pl.ds(start, depth)] for t in mine], axis=0)
                    part = jnp.dot(
                        lhs, w[row : row + depth, pl.ds(first_column, tile)], preferred_element_type=jnp.float32
                    )
                    raw = part if raw is None else raw + part
                c, s = cos_ref[base : base + n], sin_ref[base : base + n]
                first, second = raw[:, :HEAD], raw[:, HEAD:]
                second = turned(second, c, s) if queries else second.astype(jnp.bfloat16)
                out_ref[base : base + n, pl.ds(out_column, HEAD)] = turned(first, c, s)
                out_ref[base : base + n, pl.ds(out_column + HEAD, HEAD)] = second
                base += n

        if queries:

            def step(n, carry):
                at = pl.multiple_of(n * tile, tile)
                columns(at, at)
                return carry

            lax.fori_loop(0, 2, step, 0)
        else:
            columns(2 * tile, 0)

    vmem = pl.BlockSpec(memory_space=pltpu.VMEM)
    return pl.pallas_call(
        kernel,
        in_specs=[pl.BlockSpec(memory_space=pltpu.SMEM)] + [vmem] * (len(tokens) + len(flat) + 2),
        out_specs=vmem,
        out_shape=jax.ShapeDtypeStruct((rows, out_width), jnp.bfloat16),
        compiler_params=pltpu.CompilerParams(vmem_limit_bytes=PROJECT_VMEM),
        cost_estimate=pl.CostEstimate(
            flops=2 * rows * width * out_width, transcendentals=0, bytes_accessed=2 * (rows * width + width * out_width)
        ),
    )(place, *tokens, *flat, cos_table, sin_table)


def best_of(s):
    best = s[:, :HEAD]
    for lane in range(HEAD, s.shape[1], HEAD):
        best = jnp.maximum(best, s[:, lane : lane + HEAD])
    return best


def key_scores(s_ref, stacked, kv):
    at = 0
    for p in kv:
        n = p.shape[0]
        s_ref[:, at : at + n] = lax.dot_general(
            stacked, p[:, :HEAD], (((1,), (1,)), ((), ())), preferred_element_type=jnp.float32
        )
        at += n


def values_and_ones(kv):
    v = jnp.concatenate([p[:, HEAD:] for p in kv], axis=0)
    return jnp.concatenate([v, jnp.ones_like(v)], axis=1)


def weigh(scores, v):
    probs = [jnp.exp2((s - less) * LOG2E_SCALE).astype(jnp.bfloat16) for s, less in scores]
    return jnp.dot(jnp.concatenate(probs, axis=1), v, preferred_element_type=jnp.float32)


def attend_own(place, q_early, q_late, kv_early, kv_late, layout):
    heads = GROUP
    total = kv_early.shape[0] + kv_late.shape[0]
    rows = total // GROUP
    early = kv_early.shape[0]

    def kernel(place_ref, qe_ref, ql_ref, ke_ref, kl_ref, sums_ref, tops_ref, q_ref, s_ref):
        g, order = place_ref[1], pl.program_id(0)

        def sort():
            at = 0
            for j, first, n in layout:
                src = qe_ref[at : at + n] if at < early else ql_ref[at - early : at - early + n]
                q_ref[j * rows + first : j * rows + first + n] = src
                at += n

        pl.when(order == 0)(sort)
        at = pl.multiple_of(order * rows, rows)
        stacked = jnp.concatenate([q_ref[pl.ds(at, rows), h * HEAD : (h + 1) * HEAD] for h in range(heads)], axis=0)
        key_scores(s_ref, stacked, (ke_ref, kl_ref))
        v = values_and_ones((ke_ref, kl_ref))
        for h in range(heads):
            mine = slice(h * rows, (h + 1) * rows)
            scores, top, at = [], None, 0
            for j, first, n in layout:
                s = s_ref[mine, at : at + n]
                at += n
                ahead = lax.broadcasted_iota(jnp.int32, s.shape, 0) - lax.broadcasted_iota(jnp.int32, s.shape, 1)
                s = jnp.where(ahead >= ((g ^ j) - (g ^ order)) * rows + first, s, NEG)
                scores.append(s)
                top = best_of(s) if top is None else jnp.maximum(top, best_of(s))
            top = jnp.max(top, axis=1, keepdims=True)
            sums_ref[order, :, 2 * h * HEAD : 2 * (h + 1) * HEAD] = weigh([(s, top) for s in scores], v)
            tops_ref[order, :, h * HEAD : (h + 1) * HEAD] = jnp.broadcast_to(top, (rows, HEAD))

    vmem = pl.BlockSpec(memory_space=pltpu.VMEM)
    return pl.pallas_call(
        kernel,
        grid=(GROUP,),
        in_specs=[pl.BlockSpec(memory_space=pltpu.SMEM)] + [vmem] * 4,
        out_specs=[vmem] * 3,
        out_shape=[
            jax.ShapeDtypeStruct((GROUP, rows, 2 * heads * HEAD), jnp.float32),
            jax.ShapeDtypeStruct((GROUP, rows, heads * HEAD), jnp.float32),
            jax.ShapeDtypeStruct((total, heads * HEAD), jnp.bfloat16),
        ],
        scratch_shapes=[pltpu.VMEM((heads * rows, total), jnp.float32)],
        compiler_params=pltpu.CompilerParams(vmem_limit_bytes=16 << 20),
        cost_estimate=pl.CostEstimate(
            flops=8 * total * heads * HEAD * total, transcendentals=total * heads * total, bytes_accessed=3 << 20
        ),
    )(place, q_early, q_late, kv_early, kv_late)


def attend_below(place, sums, tops, queries, below, piece):
    heads = GROUP
    rows = queries.shape[0] // GROUP
    flat = [p for slab in below for p in slab]
    total = sum(p.shape[0] for p in flat)

    def kernel(place_ref, sums_ref, tops_ref, q_ref, *refs):
        kv = refs[: len(flat)]
        out_ref, s_ref = refs[len(flat) :]
        z = place_ref[0]
        first_row = piece * rows
        stacked = jnp.concatenate(
            [q_ref[first_row : first_row + rows, h * HEAD : (h + 1) * HEAD] for h in range(heads)], axis=0
        )
        key_scores(s_ref, stacked, kv)
        v = values_and_ones(kv)
        for h in range(heads):
            mine = slice(h * rows, (h + 1) * rows)
            old = tops_ref[piece, :, h * HEAD : h * HEAD + 1]
            found, top, at = [], tops_ref[piece, :, h * HEAD : (h + 1) * HEAD], 0
            for d, slab in enumerate(below, start=1):
                n = sum(p.shape[0] for p in slab)
                s = s_ref[mine, at : at + n]
                at += n
                found.append((s, z >= d))
                top = jnp.maximum(top, jnp.where(z >= d, best_of(s), NEG))
            top = jnp.max(top, axis=1, keepdims=True)
            mixed = weigh([(s, jnp.where(visible, top, -NEG)) for s, visible in found], v)
            mixed = mixed + sums_ref[piece, :, 2 * h * HEAD : 2 * (h + 1) * HEAD] * jnp.exp2((old - top) * LOG2E_SCALE)
            out_ref[:, h * HEAD : (h + 1) * HEAD] = (mixed[:, :HEAD] / mixed[:, HEAD:]).astype(jnp.bfloat16)

    vmem = pl.BlockSpec(memory_space=pltpu.VMEM)
    return pl.pallas_call(
        kernel,
        in_specs=[pl.BlockSpec(memory_space=pltpu.SMEM)] + [vmem] * (3 + len(flat)),
        out_specs=vmem,
        out_shape=jax.ShapeDtypeStruct((rows, heads * HEAD), jnp.bfloat16),
        scratch_shapes=[pltpu.VMEM((heads * rows, total), jnp.float32)],
        compiler_params=pltpu.CompilerParams(vmem_limit_bytes=28 << 20),
        cost_estimate=pl.CostEstimate(
            flops=8 * rows * heads * HEAD * total, transcendentals=rows * heads * total, bytes_accessed=3 << 20
        ),
    )(place, sums, tops, queries, *flat)


def section_tick(tokens, norm_gain, w_query, w_key, w_value):
    rank = lax.axis_index("seq")
    z, g = rank // GROUP, rank % GROUP
    place = jnp.stack([z, g]).astype(jnp.int32)
    rows = tokens.shape[1]
    half = rows // 2

    def columns(j):
        c = g ^ j
        take = lambda w, n: lax.dynamic_slice_in_dim(w[0], c * n, n, 1)
        return jnp.concatenate([take(w_query, 4 * HEAD), take(w_key, HEAD), take(w_value, HEAD)], axis=1)

    got = []
    for j in (1, 2, 3):
        got.append(near(columns(j), j))
    chip = jnp.concatenate([columns(0), got[0]], axis=0)
    other = jnp.concatenate([got[1], got[2]], axis=0)
    chip_left = along(chip, 1)
    chip_right = along(chip, -1)
    other_left = along(other, 1)
    other_right = along(other, -1)
    chip_far = along(chip_left, 1)
    other_far = along(other_right, -1)
    weights = [[chip, other], [chip_right, other_right], [chip_far, other_far], [chip_left, other_left]]

    normed = normalize(tokens[0], norm_gain[0])
    side = near(normed, 1)
    across, corner = [], []
    for i in range(2):
        across.append(near(normed[i * half : (i + 1) * half], 2))
    for i in range(2):
        corner.append(near(across[i], 1))

    early = [(0, 0, rows), (1, 0, rows), (2, 0, half), (3, 0, half)]
    late = [(2, half, half), (3, half, half)]
    tables_early = rope_tables(z, g, rows, early)
    tables_late = rope_tables(z, g, rows, late)
    chunks_early = [[normed, side, across[0], corner[0]]]
    chunks_late = [[across[1], corner[1]]]
    kv_early = project(place, chunks_early, weights, *tables_early, False)
    q_early = project(place, chunks_early, weights, *tables_early, True)
    kv_late = project(place, chunks_late, weights, *tables_late, False)
    q_late = project(place, chunks_late, weights, *tables_late, True)

    cut = kv_early.shape[0] // 2
    one = upward(kv_early, [(0, 1), (1, 2), (2, 3)])
    three = upward(kv_early, [(0, 3), (1, 0)])
    two_a = upward(one[:cut], [(1, 2), (2, 3)])
    two_b = upward(three[cut:], [(3, 2), (0, 3)])
    late_one = upward(kv_late, [(0, 1), (1, 2), (2, 3)])
    late_two = upward(kv_late, [(0, 2), (1, 3)])
    late_three = upward(kv_late, [(0, 3)])
    below = [[one, late_one], [two_a, two_b, late_two], [three, late_three]]

    sums, tops, queries = attend_own(place, q_early, q_late, kv_early, kv_late, early + late)
    out = jnp.zeros((rows, GROUP * GROUP * HEAD), jnp.bfloat16)
    for k in range(GROUP):
        mixed = attend_below(place, sums, tops, queries, below, k)
        arrived = onward(mixed, k)
        out = lax.dynamic_update_slice(out, arrived, (0, (g ^ k) * GROUP * HEAD))
    return out[None]


def solution(mesh):
    return jax.shard_map(
        section_tick,
        mesh=mesh,
        in_specs=(
            P("section", "seq", None),
            P("section", None),
            P("section", "seq", None),
            P("section", "seq", None),
            P("section", "seq", None),
        ),
        out_specs=P("section", "seq", None),
        check_vma=False,
    )
```

```python
import math

import jax
import jax.numpy as jnp
from jax import lax
from jax.experimental import pallas as pl
from jax.experimental.pallas import tpu as pltpu
from jax.sharding import PartitionSpec as P


HEAD = 128
GROUP = 4
RING = 4
LOG2E_SCALE = math.log2(math.e) / math.sqrt(HEAD)
NEG = -1e30


def near(block, bits):
    return lax.ppermute(block, "seq", [(r, r ^ bits) for r in range(RING * GROUP)])


def along(block, step):
    n = RING * GROUP
    return lax.ppermute(block, "seq", [(r, (r + step * GROUP) % n) for r in range(n)])


def upward(block, routes):
    return lax.ppermute(block, "seq", [(a * GROUP + g, b * GROUP + g) for a, b in routes for g in range(GROUP)])


def onward(block, bits):
    n = RING * GROUP
    s = lax.axis_size("section")
    route = [(i * n + r, ((i + 1) % s) * n + (r ^ bits)) for i in range(s) for r in range(n)]
    return lax.ppermute(block, ("section", "seq"), route)


def normalize(rows_in, gain_row):
    wide = rows_in.astype(jnp.float32)
    scale = lax.rsqrt(jnp.mean(wide * wide, axis=-1, keepdims=True) + 1e-05)
    return (wide * scale * gain_row.astype(jnp.float32)).astype(jnp.bfloat16)


def rope_tables(z, g, rows, pieces):
    at = [(z * GROUP + (g ^ j)) * rows + first + jnp.arange(n) for j, first, n in pieces]
    positions = jnp.concatenate(at).astype(jnp.float32)
    half = HEAD // 2
    freqs = jnp.power(jnp.float32(500000.0), -(jnp.arange(half).astype(jnp.float32) * 2.0 / HEAD))
    angles = positions[:, None] * jnp.concatenate([freqs, freqs])[None, :]
    sign = jnp.where(jnp.arange(HEAD) < half, -1.0, 1.0).astype(jnp.float32)
    return jnp.cos(angles), jnp.sin(angles) * sign[None, :]


def turned(x, c, s):
    return (x * c + pltpu.roll(x, HEAD // 2, 1) * s).astype(jnp.bfloat16)


def block_starts(place_ref, offsets, depth):
    z, g = place_ref[0], place_ref[1]
    return [
        pl.multiple_of((((z + off) % RING) * GROUP + (g ^ j)) * depth, depth) for off in offsets for j in range(GROUP)
    ]


def contract(tok, starts, wts, first_column, tile, depth):
    rows = [(w, row) for w in wts for row in range(0, w.shape[0], depth)]
    raw = None
    for start, (w, row) in zip(starts, rows, strict=True):
        lhs = jnp.concatenate([t[:, pl.ds(start, depth)] for t in tok], axis=0)
        part = jnp.dot(lhs, w[row : row + depth, pl.ds(first_column, tile)], preferred_element_type=jnp.float32)
        raw = part if raw is None else raw + part
    return raw


def put(out_ref, column, raw, c, s, turn_second):
    first, second = raw[:, :HEAD], raw[:, HEAD:]
    out_ref[:, column : column + HEAD] = turned(first, c, s)
    out_ref[:, column + HEAD : column + 2 * HEAD] = turned(second, c, s) if turn_second else second.astype(jnp.bfloat16)


def cost(rows, depth, columns):
    return pl.CostEstimate(
        flops=2 * rows * depth * columns, transcendentals=0, bytes_accessed=2 * (rows * depth + depth * columns)
    )


def vmem_call(kernel, n_in, out_shape, limit, estimate, **more):
    vmem = pl.BlockSpec(memory_space=pltpu.VMEM)
    return pl.pallas_call(
        kernel,
        in_specs=[pl.BlockSpec(memory_space=pltpu.SMEM)] + [vmem] * n_in,
        out_specs=jax.tree.map(lambda _: vmem, out_shape),
        out_shape=out_shape,
        compiler_params=pltpu.CompilerParams(vmem_limit_bytes=limit << 20),
        cost_estimate=estimate,
        **more,
    )


def project_most(place, tokens, slabs, offsets):
    rows = sum(t.shape[0] for t in tokens)
    flat = [w for slab in slabs for w in slab]
    depth = tokens[0].shape[1] // (RING * GROUP)
    held, columns = sum(w.shape[0] for w in flat), flat[0].shape[1]
    tile = 2 * HEAD

    def kernel(place_ref, *refs):
        tok, wts = refs[: len(tokens)], refs[len(tokens) : len(tokens) + len(flat)]
        raw_ref, kept_ref = refs[len(tokens) + len(flat) :]
        starts = block_starts(place_ref, offsets, depth)

        def step(n, carry):
            at = pl.multiple_of(n * tile, tile)
            raw_ref[:, pl.ds(at, tile)] = contract(tok, starts, wts, at, tile, depth)
            return carry

        lax.fori_loop(0, columns // tile, step, 0)
        at = 0
        for w in wts:
            kept_ref[at : at + w.shape[0]] = w[...]
            at += w.shape[0]

    out_shape = [
        jax.ShapeDtypeStruct((rows, columns), jnp.float32),
        jax.ShapeDtypeStruct((held, columns), jnp.bfloat16),
    ]
    return vmem_call(kernel, len(tokens) + len(flat), out_shape, 16, cost(rows, held, columns))(place, *tokens, *flat)


def project_rest(place, tokens, raw, slab, offset, tables, queries):
    rows = raw.shape[0]
    depth = tokens[0].shape[1] // (RING * GROUP)
    tile = 2 * HEAD
    first, width = (0, 2 * tile) if queries else (2 * tile, tile)

    def kernel(place_ref, *refs):
        tok, wts = refs[: len(tokens)], refs[len(tokens) : len(tokens) + len(slab)]
        raw_ref, cos_ref, sin_ref, out_ref = refs[len(tokens) + len(slab) :]
        starts = block_starts(place_ref, [offset], depth)
        for at in range(0, width, tile):
            total = contract(tok, starts, wts, first + at, tile, depth) + raw_ref[:, first + at : first + at + tile]
            put(out_ref, at, total, cos_ref[...], sin_ref[...], queries)

    out_shape = jax.ShapeDtypeStruct((rows, width), jnp.bfloat16)
    return vmem_call(kernel, len(tokens) + len(slab) + 3, out_shape, 8, cost(rows, 4 * depth, width))(
        place, *tokens, *slab, raw, *tables
    )


def project_late(place, tokens, wts, offsets, tables):
    rows = sum(t.shape[0] for t in tokens)
    depth = tokens[0].shape[1] // (RING * GROUP)
    tile = 2 * HEAD

    def kernel(place_ref, *refs):
        tok, weights = refs[: len(tokens)], refs[len(tokens) : len(tokens) + len(wts)]
        cos_ref, sin_ref, kv_ref, q_ref = refs[len(tokens) + len(wts) :]
        starts = block_starts(place_ref, offsets, depth)
        for n in range(3):
            raw = contract(tok, starts, weights, n * tile, tile, depth)
            put(q_ref if n < 2 else kv_ref, n % 2 * tile, raw, cos_ref[...], sin_ref[...], n < 2)

    out_shape = [
        jax.ShapeDtypeStruct((rows, tile), jnp.bfloat16),
        jax.ShapeDtypeStruct((rows, 2 * tile), jnp.bfloat16),
    ]
    return vmem_call(kernel, len(tokens) + len(wts) + 2, out_shape, 8, cost(rows, 16 * depth, 3 * tile))(
        place, *tokens, *wts, *tables
    )


def best_of(s):
    best = s[:, :HEAD]
    for lane in range(HEAD, s.shape[1], HEAD):
        best = jnp.maximum(best, s[:, lane : lane + HEAD])
    return best


def key_scores(s_ref, stacked, kv):
    at = 0
    for p in kv:
        n = p.shape[0]
        s_ref[:, at : at + n] = lax.dot_general(
            stacked, p[:, :HEAD], (((1,), (1,)), ((), ())), preferred_element_type=jnp.float32
        )
        at += n


def values_and_ones(kv):
    v = jnp.concatenate([p[:, HEAD:] for p in kv], axis=0)
    return jnp.concatenate([v, jnp.ones_like(v)], axis=1)


def weigh(scores, v):
    probs = [jnp.exp2((s - less) * LOG2E_SCALE).astype(jnp.bfloat16) for s, less in scores]
    return jnp.dot(jnp.concatenate(probs, axis=1), v, preferred_element_type=jnp.float32)


def attend_own(place, q_early, q_late, kv_early, kv_late, layout):
    heads = GROUP
    total = kv_early.shape[0] + kv_late.shape[0]
    rows = total // GROUP
    early = kv_early.shape[0]

    def kernel(place_ref, qe_ref, ql_ref, ke_ref, kl_ref, sums_ref, tops_ref, q_ref, s_ref):
        g, order = place_ref[1], pl.program_id(0)

        def sort():
            at = 0
            for j, first, n in layout:
                src = qe_ref[at : at + n] if at < early else ql_ref[at - early : at - early + n]
                q_ref[j * rows + first : j * rows + first + n] = src
                at += n

        pl.when(order == 0)(sort)
        at = pl.multiple_of(order * rows, rows)
        stacked = jnp.concatenate([q_ref[pl.ds(at, rows), h * HEAD : (h + 1) * HEAD] for h in range(heads)], axis=0)
        key_scores(s_ref, stacked, (ke_ref, kl_ref))
        v = values_and_ones((ke_ref, kl_ref))
        for h in range(heads):
            mine = slice(h * rows, (h + 1) * rows)
            scores, top, at = [], None, 0
            for j, first, n in layout:
                s = s_ref[mine, at : at + n]
                at += n
                ahead = lax.broadcasted_iota(jnp.int32, s.shape, 0) - lax.broadcasted_iota(jnp.int32, s.shape, 1)
                s = jnp.where(ahead >= ((g ^ j) - (g ^ order)) * rows + first, s, NEG)
                scores.append(s)
                top = best_of(s) if top is None else jnp.maximum(top, best_of(s))
            top = jnp.max(top, axis=1, keepdims=True)
            sums_ref[order, :, 2 * h * HEAD : 2 * (h + 1) * HEAD] = weigh([(s, top) for s in scores], v)
            tops_ref[order, :, h * HEAD : (h + 1) * HEAD] = jnp.broadcast_to(top, (rows, HEAD))

    vmem = pl.BlockSpec(memory_space=pltpu.VMEM)
    return pl.pallas_call(
        kernel,
        grid=(GROUP,),
        in_specs=[pl.BlockSpec(memory_space=pltpu.SMEM)] + [vmem] * 4,
        out_specs=[vmem] * 3,
        out_shape=[
            jax.ShapeDtypeStruct((GROUP, rows, 2 * heads * HEAD), jnp.float32),
            jax.ShapeDtypeStruct((GROUP, rows, heads * HEAD), jnp.float32),
            jax.ShapeDtypeStruct((total, heads * HEAD), jnp.bfloat16),
        ],
        scratch_shapes=[pltpu.VMEM((heads * rows, total), jnp.float32)],
        compiler_params=pltpu.CompilerParams(vmem_limit_bytes=16 << 20),
        cost_estimate=pl.CostEstimate(
            flops=8 * total * heads * HEAD * total, transcendentals=total * heads * total, bytes_accessed=3 << 20
        ),
    )(place, q_early, q_late, kv_early, kv_late)


def attend_below(place, sums, tops, queries, below, piece):
    heads = GROUP
    rows = queries.shape[0] // GROUP
    flat = [p for slab in below for p in slab]
    total = sum(p.shape[0] for p in flat)

    def kernel(place_ref, sums_ref, tops_ref, q_ref, *refs):
        kv = refs[: len(flat)]
        out_ref, s_ref = refs[len(flat) :]
        z = place_ref[0]
        first_row = piece * rows
        stacked = jnp.concatenate(
            [q_ref[first_row : first_row + rows, h * HEAD : (h + 1) * HEAD] for h in range(heads)], axis=0
        )
        key_scores(s_ref, stacked, kv)
        v = values_and_ones(kv)
        for h in range(heads):
            mine = slice(h * rows, (h + 1) * rows)
            old = tops_ref[piece, :, h * HEAD : (h + 1) * HEAD]
            found, top, at = [], old, 0
            for d, slab in enumerate(below, start=1):
                n = sum(p.shape[0] for p in slab)
                s = s_ref[mine, at : at + n]
                at += n
                found.append((s, z >= d))
                top = jnp.maximum(top, jnp.where(z >= d, best_of(s), NEG))
            top = jnp.max(top, axis=1, keepdims=True)
            mixed = weigh([(s, jnp.where(visible, top, -NEG)) for s, visible in found], v)
            shrink = jnp.exp2((old - top) * LOG2E_SCALE)
            at = 2 * h * HEAD
            above = mixed[:, :HEAD] + sums_ref[piece, :, at : at + HEAD] * shrink
            under = mixed[:, HEAD:] + sums_ref[piece, :, at + HEAD : at + 2 * HEAD] * shrink
            out_ref[:, h * HEAD : (h + 1) * HEAD] = (above / under).astype(jnp.bfloat16)

    vmem = pl.BlockSpec(memory_space=pltpu.VMEM)
    return pl.pallas_call(
        kernel,
        in_specs=[pl.BlockSpec(memory_space=pltpu.SMEM)] + [vmem] * (3 + len(flat)),
        out_specs=vmem,
        out_shape=jax.ShapeDtypeStruct((rows, heads * HEAD), jnp.bfloat16),
        scratch_shapes=[pltpu.VMEM((heads * rows, total), jnp.float32)],
        compiler_params=pltpu.CompilerParams(vmem_limit_bytes=28 << 20),
        cost_estimate=pl.CostEstimate(
            flops=8 * rows * heads * HEAD * total, transcendentals=rows * heads * total, bytes_accessed=3 << 20
        ),
    )(place, sums, tops, queries, *flat)


def section_tick(tokens, norm_gain, w_query, w_key, w_value):
    rank = lax.axis_index("seq")
    z, g = rank // GROUP, rank % GROUP
    place = jnp.stack([z, g]).astype(jnp.int32)
    rows = tokens.shape[1]
    half = rows // 2

    def columns(j):
        c = g ^ j
        take = lambda w, n: lax.dynamic_slice_in_dim(w[0], c * n, n, 1)
        return jnp.concatenate([take(w_query, 4 * HEAD), take(w_key, HEAD), take(w_value, HEAD)], axis=1)

    got = []
    for j in (1, 2, 3):
        got.append(near(columns(j), j))
    chip = jnp.concatenate([columns(0), got[0]], axis=0)
    other = jnp.concatenate([got[1], got[2]], axis=0)
    chip_left = along(chip, 1)
    chip_right = along(chip, -1)
    other_left = along(other, 1)
    other_right = along(other, -1)
    chip_far = along(chip_left, 1)
    other_far = along(other_right, -1)
    most = [[chip, other], [chip_right, other_right], [chip_left, other_left]]
    far = [chip_far, other_far]

    normed = normalize(tokens[0], norm_gain[0])
    side = near(normed, 1)
    across, corner = [], []
    for i in range(2):
        across.append(near(normed[i * half : (i + 1) * half], 2))
    for i in range(2):
        corner.append(near(across[i], 1))

    early = [(0, 0, rows), (1, 0, rows), (2, 0, half), (3, 0, half)]
    late = [(2, half, half), (3, half, half)]
    tables_early = rope_tables(z, g, rows, early)
    tables_late = rope_tables(z, g, rows, late)
    tokens_early = [normed, side, across[0], corner[0]]
    raw, kept = project_most(place, tokens_early, most, (0, 1, 3))
    kv_early = project_rest(place, tokens_early, raw, far, 2, tables_early, False)
    q_early = project_rest(place, tokens_early, raw, far, 2, tables_early, True)
    kv_late, q_late = project_late(place, [across[1], corner[1]], [kept, *far], (0, 1, 3, 2), tables_late)

    below = [[], [], []]
    for kv in (kv_early, kv_late):
        for d in (1, 2, 3):
            below[d - 1].append(upward(kv, [(z0, z0 + d) for z0 in range(RING - d)]))

    sums, tops, queries = attend_own(place, q_early, q_late, kv_early, kv_late, early + late)
    out = jnp.zeros((rows, GROUP * GROUP * HEAD), jnp.bfloat16)
    for k in range(GROUP):
        mixed = attend_below(place, sums, tops, queries, below, k)
        arrived = onward(mixed, k)
        out = lax.dynamic_update_slice(out, arrived, (0, (g ^ k) * GROUP * HEAD))
    return out[None]


def solution(mesh):
    return jax.shard_map(
        section_tick,
        mesh=mesh,
        in_specs=(
            P("section", "seq", None),
            P("section", None),
            P("section", "seq", None),
            P("section", "seq", None),
            P("section", "seq", None),
        ),
        out_specs=P("section", "seq", None),
        check_vma=False,
    )
```

```python
import math

import jax
import jax.numpy as jnp
from jax import lax
from jax.experimental import pallas as pl
from jax.experimental.pallas import tpu as pltpu
from jax.sharding import PartitionSpec as P


HEAD = 128
GROUP = 4
RING = 4
LOG2E_SCALE = math.log2(math.e) / math.sqrt(HEAD)
NEG = -1e30


def near(block, bits):
    return lax.ppermute(block, "seq", [(r, r ^ bits) for r in range(RING * GROUP)])


def along(block, step):
    n = RING * GROUP
    return lax.ppermute(block, "seq", [(r, (r + step * GROUP) % n) for r in range(n)])


def upward(block, routes):
    return lax.ppermute(block, "seq", [(a * GROUP + g, b * GROUP + g) for a, b in routes for g in range(GROUP)])


def onward(block, bits):
    n = RING * GROUP
    s = lax.axis_size("section")
    route = [(i * n + r, ((i + 1) % s) * n + (r ^ bits)) for i in range(s) for r in range(n)]
    return lax.ppermute(block, ("section", "seq"), route)


def normalize(tokens, gain_row):
    rows, width = tokens.shape
    step_rows, half = 32, rows // 2

    def kernel(x_ref, gain_ref, whole_ref, low_ref, high_ref):
        gain = gain_ref[...].astype(jnp.float32)

        def step(i, carry):
            mine = pl.ds(pl.multiple_of(i * step_rows, step_rows), step_rows)
            wide = x_ref[mine].astype(jnp.float32)
            scale = lax.rsqrt(jnp.mean(wide * wide, axis=-1, keepdims=True) + 1e-05)
            whole_ref[mine] = (wide * scale * gain).astype(jnp.bfloat16)
            return carry

        lax.fori_loop(0, rows // step_rows, step, 0)
        low_ref[...] = whole_ref[:half]
        high_ref[...] = whole_ref[half:]

    vmem = pl.BlockSpec(memory_space=pltpu.VMEM)
    part = jax.ShapeDtypeStruct((half, width), jnp.bfloat16)
    return pl.pallas_call(
        kernel,
        in_specs=[vmem, vmem],
        out_specs=[vmem] * 3,
        out_shape=[jax.ShapeDtypeStruct((rows, width), jnp.bfloat16), part, part],
        compiler_params=pltpu.CompilerParams(vmem_limit_bytes=12 << 20),
        cost_estimate=pl.CostEstimate(flops=4 * rows * width, transcendentals=rows, bytes_accessed=6 * rows * width),
    )(tokens, gain_row)


def rope_tables(z, g, rows, pieces):
    at = [(z * GROUP + (g ^ j)) * rows + first + jnp.arange(n) for j, first, n in pieces]
    positions = jnp.concatenate(at).astype(jnp.float32)
    half = HEAD // 2
    freqs = jnp.power(jnp.float32(500000.0), -(jnp.arange(half).astype(jnp.float32) * 2.0 / HEAD))
    angles = positions[:, None] * jnp.concatenate([freqs, freqs])[None, :]
    sign = jnp.where(jnp.arange(HEAD) < half, -1.0, 1.0).astype(jnp.float32)
    return jnp.cos(angles), jnp.sin(angles) * sign[None, :]


def turned(x, c, s):
    return (x * c + pltpu.roll(x, HEAD // 2, 1) * s).astype(jnp.bfloat16)


def block_starts(place_ref, offsets, depth):
    z, g = place_ref[0], place_ref[1]
    return [
        pl.multiple_of((((z + off) % RING) * GROUP + (g ^ j)) * depth, depth) for off in offsets for j in range(GROUP)
    ]


def contract(tok, starts, wts, column, tile, depth):
    rows = [(w, base, row) for w, base in wts for row in range(0, w.shape[0], depth)]
    raw = None
    for start, (w, base, row) in zip(starts, rows, strict=True):
        lhs = jnp.concatenate([t[:, pl.ds(start, depth)] for t in tok], axis=0)
        part = jnp.dot(lhs, w[row : row + depth, pl.ds(base + column, tile)], preferred_element_type=jnp.float32)
        raw = part if raw is None else raw + part
    return raw


def put(out_ref, column, raw, c, s, turn_second):
    first, second = raw[:, :HEAD], raw[:, HEAD:]
    out_ref[:, pl.ds(column, HEAD)] = turned(first, c, s)
    out_ref[:, pl.ds(column + HEAD, HEAD)] = turned(second, c, s) if turn_second else second.astype(jnp.bfloat16)


def cost(rows, depth, columns):
    return pl.CostEstimate(
        flops=2 * rows * depth * columns, transcendentals=0, bytes_accessed=2 * (rows * depth + depth * columns)
    )


def vmem_call(kernel, n_in, out_shape, limit, estimate, **more):
    vmem = pl.BlockSpec(memory_space=pltpu.VMEM)
    return pl.pallas_call(
        kernel,
        in_specs=[pl.BlockSpec(memory_space=pltpu.SMEM)] + [vmem] * n_in,
        out_specs=jax.tree.map(lambda _: vmem, out_shape),
        out_shape=out_shape,
        compiler_params=pltpu.CompilerParams(vmem_limit_bytes=limit << 20),
        cost_estimate=estimate,
        **more,
    )


def pack(kept_ref, wts, width):
    at = 0
    for w, base in wts:
        kept_ref[at : at + w.shape[0]] = w[:, base : base + width]
        at += w.shape[0]


def project_kv(place, tokens, wts, bases, offsets, tables):
    rows = sum(t.shape[0] for t in tokens)
    depth = tokens[0].shape[1] // (RING * GROUP)
    held, tile = sum(w.shape[0] for w in wts), 2 * HEAD

    def kernel(place_ref, *refs):
        tok, weights = refs[: len(tokens)], list(zip(refs[len(tokens) :], bases))
        cos_ref, sin_ref, kv_ref, kept_ref = refs[len(tokens) + len(wts) :]
        raw = contract(tok, block_starts(place_ref, offsets, depth), weights, 0, tile, depth)
        put(kv_ref, 0, raw, cos_ref[:rows], sin_ref[:rows], False)
        pack(kept_ref, weights, tile)

    out_shape = [
        jax.ShapeDtypeStruct((rows, tile), jnp.bfloat16),
        jax.ShapeDtypeStruct((held, tile), jnp.bfloat16),
    ]
    return vmem_call(kernel, len(tokens) + len(wts) + 2, out_shape, 16, cost(rows, held, tile))(
        place, *tokens, *wts, *tables
    )


def project_most(place, tokens, wts, offsets):
    rows = sum(t.shape[0] for t in tokens)
    depth = tokens[0].shape[1] // (RING * GROUP)
    held, tile = sum(w.shape[0] for w in wts), 2 * HEAD

    def kernel(place_ref, *refs):
        tok, weights = refs[: len(tokens)], [(w, 0) for w in refs[len(tokens) : len(tokens) + len(wts)]]
        raw_ref, kept_ref = refs[len(tokens) + len(wts) :]
        starts = block_starts(place_ref, offsets, depth)

        def step(n, carry):
            at = pl.multiple_of(n * tile, tile)
            raw_ref[:, pl.ds(at, tile)] = contract(tok, starts, weights, at, tile, depth)
            return carry

        lax.fori_loop(0, 2, step, 0)
        pack(kept_ref, weights, 2 * tile)

    out_shape = [
        jax.ShapeDtypeStruct((rows, 2 * tile), jnp.float32),
        jax.ShapeDtypeStruct((held, 2 * tile), jnp.bfloat16),
    ]
    return vmem_call(kernel, len(tokens) + len(wts), out_shape, 16, cost(rows, held, 2 * tile))(place, *tokens, *wts)


def project_rest(place, tokens, raw, slab, offset, tables):
    rows = raw.shape[0]
    depth = tokens[0].shape[1] // (RING * GROUP)
    tile = 2 * HEAD

    def kernel(place_ref, *refs):
        tok, wts = refs[: len(tokens)], [(w, 0) for w in refs[len(tokens) : len(tokens) + len(slab)]]
        raw_ref, cos_ref, sin_ref, out_ref = refs[len(tokens) + len(slab) :]
        starts = block_starts(place_ref, [offset], depth)

        def step(n, carry):
            at = pl.multiple_of(n * tile, tile)
            total = contract(tok, starts, wts, at, tile, depth) + raw_ref[:, pl.ds(at, tile)]
            put(out_ref, at, total, cos_ref[:rows], sin_ref[:rows], True)
            return carry

        lax.fori_loop(0, 2, step, 0)

    out_shape = jax.ShapeDtypeStruct((rows, 2 * tile), jnp.bfloat16)
    return vmem_call(kernel, len(tokens) + len(slab) + 3, out_shape, 8, cost(rows, 4 * depth, 2 * tile))(
        place, *tokens, *slab, raw, *tables
    )


def project_late(place, tokens, kv_weights, q_weights, offsets, tables):
    rows = sum(t.shape[0] for t in tokens)
    depth = tokens[0].shape[1] // (RING * GROUP)
    tile = 2 * HEAD
    n, first = len(tokens), tables[0].shape[0] - rows

    def kernel(place_ref, *refs):
        tok, kvw = refs[:n], [(refs[n], 0)]
        qw = [(w, 0) for w in refs[n + 1 : n + 1 + len(q_weights)]]
        cos_ref, sin_ref, kv_ref, q_ref = refs[n + 1 + len(q_weights) :]
        starts = block_starts(place_ref, offsets, depth)
        raw = contract(tok, starts, kvw, 0, tile, depth)
        put(kv_ref, 0, raw, cos_ref[first:], sin_ref[first:], False)

        def step(n, carry):
            at = pl.multiple_of(n * tile, tile)
            put(q_ref, at, contract(tok, starts, qw, at, tile, depth), cos_ref[first:], sin_ref[first:], True)
            return carry

        lax.fori_loop(0, 2, step, 0)

    out_shape = [
        jax.ShapeDtypeStruct((rows, tile), jnp.bfloat16),
        jax.ShapeDtypeStruct((rows, 2 * tile), jnp.bfloat16),
    ]
    return vmem_call(kernel, n + 1 + len(q_weights) + 2, out_shape, 8, cost(rows, 16 * depth, 3 * tile))(
        place, *tokens, kv_weights, *q_weights, *tables
    )


def best_of(s):
    best = s[:, :HEAD]
    for lane in range(HEAD, s.shape[1], HEAD):
        best = jnp.maximum(best, s[:, lane : lane + HEAD])
    return best


def key_scores(s_ref, stacked, kv):
    at = 0
    for p in kv:
        n = p.shape[0]
        s_ref[:, at : at + n] = lax.dot_general(
            stacked, p[:, :HEAD], (((1,), (1,)), ((), ())), preferred_element_type=jnp.float32
        )
        at += n


def values_and_ones(kv):
    v = jnp.concatenate([p[:, HEAD:] for p in kv], axis=0)
    return jnp.concatenate([v, jnp.ones_like(v)], axis=1)


def weigh(scores, v):
    probs = [jnp.exp2((s - less) * LOG2E_SCALE).astype(jnp.bfloat16) for s, less in scores]
    return jnp.dot(jnp.concatenate(probs, axis=1), v, preferred_element_type=jnp.float32)


def attend_own(place, q_early, q_late, kv_early, kv_late, layout):
    heads = GROUP
    total = kv_early.shape[0] + kv_late.shape[0]
    rows = total // GROUP
    early = kv_early.shape[0]

    def kernel(place_ref, qe_ref, ql_ref, ke_ref, kl_ref, sums_ref, tops_ref, q_ref, s_ref):
        g, order = place_ref[1], pl.program_id(0)

        def sort():
            at = 0
            for j, first, n in layout:
                src = qe_ref[at : at + n] if at < early else ql_ref[at - early : at - early + n]
                q_ref[j * rows + first : j * rows + first + n] = src
                at += n

        pl.when(order == 0)(sort)
        at = pl.multiple_of(order * rows, rows)
        stacked = jnp.concatenate([q_ref[pl.ds(at, rows), h * HEAD : (h + 1) * HEAD] for h in range(heads)], axis=0)
        key_scores(s_ref, stacked, (ke_ref, kl_ref))
        v = values_and_ones((ke_ref, kl_ref))
        for h in range(heads):
            mine = slice(h * rows, (h + 1) * rows)
            scores, top, at = [], None, 0
            for j, first, n in layout:
                s = s_ref[mine, at : at + n]
                at += n
                ahead = lax.broadcasted_iota(jnp.int32, s.shape, 0) - lax.broadcasted_iota(jnp.int32, s.shape, 1)
                s = jnp.where(ahead >= ((g ^ j) - (g ^ order)) * rows + first, s, NEG)
                scores.append(s)
                top = best_of(s) if top is None else jnp.maximum(top, best_of(s))
            top = jnp.max(top, axis=1, keepdims=True)
            sums_ref[order, :, 2 * h * HEAD : 2 * (h + 1) * HEAD] = weigh([(s, top) for s in scores], v)
            tops_ref[order, :, h * HEAD : (h + 1) * HEAD] = jnp.broadcast_to(top, (rows, HEAD))

    vmem = pl.BlockSpec(memory_space=pltpu.VMEM)
    return pl.pallas_call(
        kernel,
        grid=(GROUP,),
        in_specs=[pl.BlockSpec(memory_space=pltpu.SMEM)] + [vmem] * 4,
        out_specs=[vmem] * 3,
        out_shape=[
            jax.ShapeDtypeStruct((GROUP, rows, 2 * heads * HEAD), jnp.float32),
            jax.ShapeDtypeStruct((GROUP, rows, heads * HEAD), jnp.float32),
            jax.ShapeDtypeStruct((total, heads * HEAD), jnp.bfloat16),
        ],
        scratch_shapes=[pltpu.VMEM((heads * rows, total), jnp.float32)],
        compiler_params=pltpu.CompilerParams(vmem_limit_bytes=16 << 20),
        cost_estimate=pl.CostEstimate(
            flops=8 * total * heads * HEAD * total, transcendentals=total * heads * total, bytes_accessed=3 << 20
        ),
    )(place, q_early, q_late, kv_early, kv_late)


def attend_below(place, sums, tops, queries, below, piece):
    heads = GROUP
    rows = queries.shape[0] // GROUP
    flat = [p for slab in below for p in slab]
    total = sum(p.shape[0] for p in flat)

    def kernel(place_ref, sums_ref, tops_ref, q_ref, *refs):
        kv = refs[: len(flat)]
        out_ref, s_ref = refs[len(flat) :]
        z = place_ref[0]
        first_row = piece * rows
        stacked = jnp.concatenate(
            [q_ref[first_row : first_row + rows, h * HEAD : (h + 1) * HEAD] for h in range(heads)], axis=0
        )
        key_scores(s_ref, stacked, kv)
        v = values_and_ones(kv)
        for h in range(heads):
            mine = slice(h * rows, (h + 1) * rows)
            old = tops_ref[piece, :, h * HEAD : (h + 1) * HEAD]
            found, top, at = [], old, 0
            for d, slab in enumerate(below, start=1):
                n = sum(p.shape[0] for p in slab)
                s = s_ref[mine, at : at + n]
                at += n
                found.append((s, z >= d))
                top = jnp.maximum(top, jnp.where(z >= d, best_of(s), NEG))
            top = jnp.max(top, axis=1, keepdims=True)
            mixed = weigh([(s, jnp.where(visible, top, -NEG)) for s, visible in found], v)
            shrink = jnp.exp2((old - top) * LOG2E_SCALE)
            at = 2 * h * HEAD
            above = mixed[:, :HEAD] + sums_ref[piece, :, at : at + HEAD] * shrink
            under = mixed[:, HEAD:] + sums_ref[piece, :, at + HEAD : at + 2 * HEAD] * shrink
            out_ref[:, h * HEAD : (h + 1) * HEAD] = (above / under).astype(jnp.bfloat16)

    vmem = pl.BlockSpec(memory_space=pltpu.VMEM)
    return pl.pallas_call(
        kernel,
        in_specs=[pl.BlockSpec(memory_space=pltpu.SMEM)] + [vmem] * (3 + len(flat)),
        out_specs=vmem,
        out_shape=jax.ShapeDtypeStruct((rows, heads * HEAD), jnp.bfloat16),
        scratch_shapes=[pltpu.VMEM((heads * rows, total), jnp.float32)],
        compiler_params=pltpu.CompilerParams(vmem_limit_bytes=28 << 20),
        cost_estimate=pl.CostEstimate(
            flops=8 * rows * heads * HEAD * total, transcendentals=rows * heads * total, bytes_accessed=3 << 20
        ),
    )(place, sums, tops, queries, *flat)


def section_tick(tokens, norm_gain, w_query, w_key, w_value):
    rank = lax.axis_index("seq")
    z, g = rank // GROUP, rank % GROUP
    place = jnp.stack([z, g]).astype(jnp.int32)
    rows = tokens.shape[1]
    half = rows // 2

    def columns(j):
        c = g ^ j
        take = lambda w, n: lax.dynamic_slice_in_dim(w[0], c * n, n, 1)
        return jnp.concatenate([take(w_query, 4 * HEAD), take(w_key, HEAD), take(w_value, HEAD)], axis=1)

    got = []
    for j in (1, 2, 3):
        got.append(near(columns(j), j))
    nq = GROUP * HEAD
    chip = jnp.concatenate([columns(0), got[0]], axis=0)
    other_kv = jnp.concatenate([got[1][:, nq:], got[2][:, nq:]], axis=0)
    other_q = jnp.concatenate([got[1][:, :nq], got[2][:, :nq]], axis=0)

    chip_left, chip_right = along(chip, 1), along(chip, -1)
    kv_left, kv_right = along(other_kv, 1), along(other_kv, -1)
    q_left, q_right = along(other_q, 1), along(other_q, -1)
    chip_far, kv_far, q_far = along(chip_left, 1), along(kv_right, -1), along(q_right, -1)
    offsets = (0, 1, 3, 2)
    kv_weights = [chip, other_kv, chip_right, kv_right, chip_left, kv_left, chip_far, kv_far]
    kv_bases = [nq, 0] * RING
    q_weights = [chip, other_q, chip_right, q_right, chip_left, q_left]

    normed, *halves = normalize(tokens[0], norm_gain)
    side = near(normed, 1)
    across, corner = [], []
    for i in range(2):
        across.append(near(halves[i], 2))
    for i in range(2):
        corner.append(near(across[i], 1))

    early = [(0, 0, rows), (1, 0, rows), (2, 0, half), (3, 0, half)]
    late = [(2, half, half), (3, half, half)]
    tables = rope_tables(z, g, rows, early + late)
    tokens_early = [normed, side, across[0], corner[0]]
    kv_early, kept_kv = project_kv(place, tokens_early, kv_weights, kv_bases, offsets, tables)
    raw, kept_q = project_most(place, tokens_early, q_weights, offsets[:3])
    q_early = project_rest(place, tokens_early, raw, [chip_far, q_far], offsets[3], tables)
    kv_late, q_late = project_late(place, [across[1], corner[1]], kept_kv, [kept_q, chip_far, q_far], offsets, tables)

    below = [[], [], []]
    for kv in (kv_early, kv_late):
        for d in (3, 2, 1):
            below[d - 1].append(upward(kv, [(z0, z0 + d) for z0 in range(RING - d)]))

    sums, tops, queries = attend_own(place, q_early, q_late, kv_early, kv_late, early + late)
    out = jnp.zeros((rows, GROUP * GROUP * HEAD), jnp.bfloat16)
    for k in range(GROUP):
        mixed = attend_below(place, sums, tops, queries, below, k)
        arrived = onward(mixed, k)
        out = lax.dynamic_update_slice(out, arrived, (0, (g ^ k) * GROUP * HEAD))
    return out[None]


def solution(mesh):
    return jax.shard_map(
        section_tick,
        mesh=mesh,
        in_specs=(
            P("section", "seq", None),
            P("section", None),
            P("section", "seq", None),
            P("section", "seq", None),
            P("section", "seq", None),
        ),
        out_specs=P("section", "seq", None),
        check_vma=False,
    )
```

```python
import math

import jax
import jax.numpy as jnp
from jax import lax
from jax.experimental import pallas as pl
from jax.experimental.pallas import tpu as pltpu
from jax.sharding import PartitionSpec as P


HEAD = 128
GROUP = 4
RING = 4
LOG2E_SCALE = math.log2(math.e) / math.sqrt(HEAD)
NEG = -1e30


def near(block, bits):
    return lax.ppermute(block, "seq", [(r, r ^ bits) for r in range(RING * GROUP)])


def along(block, step):
    n = RING * GROUP
    return lax.ppermute(block, "seq", [(r, (r + step * GROUP) % n) for r in range(n)])


def upward(block, routes):
    return lax.ppermute(block, "seq", [(a * GROUP + g, b * GROUP + g) for a, b in routes for g in range(GROUP)])


def onward(block, bits):
    n = RING * GROUP
    s = lax.axis_size("section")
    route = [(i * n + r, ((i + 1) % s) * n + (r ^ bits)) for i in range(s) for r in range(n)]
    return lax.ppermute(block, ("section", "seq"), route)


def normalize(tokens, gain_row):
    rows, width = tokens.shape
    step_rows, half = 32, rows // 2

    def kernel(x_ref, gain_ref, whole_ref, low_ref, high_ref):
        gain = gain_ref[...].astype(jnp.float32)

        def step(i, carry):
            mine = pl.ds(pl.multiple_of(i * step_rows, step_rows), step_rows)
            wide = x_ref[mine].astype(jnp.float32)
            scale = lax.rsqrt(jnp.mean(wide * wide, axis=-1, keepdims=True) + 1e-05)
            whole_ref[mine] = (wide * scale * gain).astype(jnp.bfloat16)
            return carry

        lax.fori_loop(0, rows // step_rows, step, 0)
        low_ref[...] = whole_ref[:half]
        high_ref[...] = whole_ref[half:]

    vmem = pl.BlockSpec(memory_space=pltpu.VMEM)
    part = jax.ShapeDtypeStruct((half, width), jnp.bfloat16)
    return pl.pallas_call(
        kernel,
        in_specs=[vmem, vmem],
        out_specs=[vmem] * 3,
        out_shape=[jax.ShapeDtypeStruct((rows, width), jnp.bfloat16), part, part],
        compiler_params=pltpu.CompilerParams(vmem_limit_bytes=12 << 20),
        cost_estimate=pl.CostEstimate(flops=4 * rows * width, transcendentals=rows, bytes_accessed=6 * rows * width),
    )(tokens, gain_row)


def rope_tables(z, g, rows, pieces):
    at = [(z * GROUP + (g ^ j)) * rows + first + jnp.arange(n) for j, first, n in pieces]
    positions = jnp.concatenate(at).astype(jnp.float32)
    half = HEAD // 2
    freqs = jnp.power(jnp.float32(500000.0), -(jnp.arange(half).astype(jnp.float32) * 2.0 / HEAD))
    angles = positions[:, None] * jnp.concatenate([freqs, freqs])[None, :]
    sign = jnp.where(jnp.arange(HEAD) < half, -1.0, 1.0).astype(jnp.float32)
    return jnp.cos(angles), jnp.sin(angles) * sign[None, :]


def turned(x, c, s):
    return (x * c + pltpu.roll(x, HEAD // 2, 1) * s).astype(jnp.bfloat16)


def block_starts(place_ref, offsets, depth):
    z, g = place_ref[0], place_ref[1]
    return [
        pl.multiple_of((((z + off) % RING) * GROUP + (g ^ j)) * depth, depth) for off in offsets for j in range(GROUP)
    ]


def contract(tok, starts, wts, column, tile, depth):
    rows = [(w, base, row) for w, base in wts for row in range(0, w.shape[0], depth)]
    raw = None
    for start, (w, base, row) in zip(starts, rows, strict=True):
        lhs = jnp.concatenate([t[:, pl.ds(start, depth)] for t in tok], axis=0)
        part = jnp.dot(lhs, w[row : row + depth, pl.ds(base + column, tile)], preferred_element_type=jnp.float32)
        raw = part if raw is None else raw + part
    return raw


def put(out_ref, column, raw, c, s, turn_second):
    first, second = raw[:, :HEAD], raw[:, HEAD:]
    out_ref[:, pl.ds(column, HEAD)] = turned(first, c, s)
    out_ref[:, pl.ds(column + HEAD, HEAD)] = turned(second, c, s) if turn_second else second.astype(jnp.bfloat16)


def cost(rows, depth, columns):
    return pl.CostEstimate(
        flops=2 * rows * depth * columns, transcendentals=0, bytes_accessed=2 * (rows * depth + depth * columns)
    )


def vmem_call(kernel, n_in, out_shape, limit, estimate, **more):
    vmem = pl.BlockSpec(memory_space=pltpu.VMEM)
    return pl.pallas_call(
        kernel,
        in_specs=[pl.BlockSpec(memory_space=pltpu.SMEM)] + [vmem] * n_in,
        out_specs=jax.tree.map(lambda _: vmem, out_shape),
        out_shape=out_shape,
        compiler_params=pltpu.CompilerParams(vmem_limit_bytes=limit << 20),
        cost_estimate=estimate,
        **more,
    )


def pack(kept_ref, wts, width):
    at = 0
    for w, base in wts:
        kept_ref[at : at + w.shape[0]] = w[:, base : base + width]
        at += w.shape[0]


def project_kv(place, tokens, wts, bases, offsets, tables):
    rows = sum(t.shape[0] for t in tokens)
    depth = tokens[0].shape[1] // (RING * GROUP)
    held, tile = sum(w.shape[0] for w in wts), 2 * HEAD

    def kernel(place_ref, *refs):
        tok, weights = refs[: len(tokens)], list(zip(refs[len(tokens) :], bases))
        cos_ref, sin_ref, kv_ref, kept_ref = refs[len(tokens) + len(wts) :]
        raw = contract(tok, block_starts(place_ref, offsets, depth), weights, 0, tile, depth)
        put(kv_ref, 0, raw, cos_ref[:rows], sin_ref[:rows], False)
        pack(kept_ref, weights, tile)

    out_shape = [
        jax.ShapeDtypeStruct((rows, tile), jnp.bfloat16),
        jax.ShapeDtypeStruct((held, tile), jnp.bfloat16),
    ]
    return vmem_call(kernel, len(tokens) + len(wts) + 2, out_shape, 16, cost(rows, held, tile))(
        place, *tokens, *wts, *tables
    )


def project_most(place, tokens, wts, offsets):
    rows = sum(t.shape[0] for t in tokens)
    depth = tokens[0].shape[1] // (RING * GROUP)
    held, tile = sum(w.shape[0] for w in wts), 2 * HEAD

    def kernel(place_ref, *refs):
        tok, weights = refs[: len(tokens)], [(w, 0) for w in refs[len(tokens) : len(tokens) + len(wts)]]
        raw_ref, kept_ref = refs[len(tokens) + len(wts) :]
        starts = block_starts(place_ref, offsets, depth)

        def step(n, carry):
            at = pl.multiple_of(n * tile, tile)
            raw_ref[:, pl.ds(at, tile)] = contract(tok, starts, weights, at, tile, depth)
            return carry

        lax.fori_loop(0, 2, step, 0)
        pack(kept_ref, weights, 2 * tile)

    out_shape = [
        jax.ShapeDtypeStruct((rows, 2 * tile), jnp.float32),
        jax.ShapeDtypeStruct((held, 2 * tile), jnp.bfloat16),
    ]
    return vmem_call(kernel, len(tokens) + len(wts), out_shape, 16, cost(rows, held, 2 * tile))(place, *tokens, *wts)


def project_rest(place, tokens, raw, slab, offset, tables):
    rows = raw.shape[0]
    depth = tokens[0].shape[1] // (RING * GROUP)
    tile = 2 * HEAD

    def kernel(place_ref, *refs):
        tok, wts = refs[: len(tokens)], [(w, 0) for w in refs[len(tokens) : len(tokens) + len(slab)]]
        raw_ref, cos_ref, sin_ref, out_ref = refs[len(tokens) + len(slab) :]
        starts = block_starts(place_ref, [offset], depth)

        def step(n, carry):
            at = pl.multiple_of(n * tile, tile)
            total = contract(tok, starts, wts, at, tile, depth) + raw_ref[:, pl.ds(at, tile)]
            put(out_ref, at, total, cos_ref[:rows], sin_ref[:rows], True)
            return carry

        lax.fori_loop(0, 2, step, 0)

    out_shape = jax.ShapeDtypeStruct((rows, 2 * tile), jnp.bfloat16)
    return vmem_call(kernel, len(tokens) + len(slab) + 3, out_shape, 8, cost(rows, 4 * depth, 2 * tile))(
        place, *tokens, *slab, raw, *tables
    )


def project_late(place, tokens, kv_weights, q_weights, offsets, tables):
    rows = sum(t.shape[0] for t in tokens)
    depth = tokens[0].shape[1] // (RING * GROUP)
    tile = 2 * HEAD
    n, first = len(tokens), tables[0].shape[0] - rows

    def kernel(place_ref, *refs):
        tok, kvw = refs[:n], [(refs[n], 0)]
        qw = [(w, 0) for w in refs[n + 1 : n + 1 + len(q_weights)]]
        cos_ref, sin_ref, kv_ref, q_ref = refs[n + 1 + len(q_weights) :]
        starts = block_starts(place_ref, offsets, depth)
        raw = contract(tok, starts, kvw, 0, tile, depth)
        put(kv_ref, 0, raw, cos_ref[first:], sin_ref[first:], False)

        def step(n, carry):
            at = pl.multiple_of(n * tile, tile)
            put(q_ref, at, contract(tok, starts, qw, at, tile, depth), cos_ref[first:], sin_ref[first:], True)
            return carry

        lax.fori_loop(0, 2, step, 0)

    out_shape = [
        jax.ShapeDtypeStruct((rows, tile), jnp.bfloat16),
        jax.ShapeDtypeStruct((rows, 2 * tile), jnp.bfloat16),
    ]
    return vmem_call(kernel, n + 1 + len(q_weights) + 2, out_shape, 8, cost(rows, 16 * depth, 3 * tile))(
        place, *tokens, kv_weights, *q_weights, *tables
    )


def best_of(s):
    best = s[:, :HEAD]
    for lane in range(HEAD, s.shape[1], HEAD):
        best = jnp.maximum(best, s[:, lane : lane + HEAD])
    return best


def key_scores(s_ref, stacked, kv):
    at = 0
    for p in kv:
        n = p.shape[0]
        s_ref[:, at : at + n] = lax.dot_general(
            stacked, p[:, :HEAD], (((1,), (1,)), ((), ())), preferred_element_type=jnp.float32
        )
        at += n


def values_and_ones(kv):
    v = jnp.concatenate([p[:, HEAD:] for p in kv], axis=0)
    return jnp.concatenate([v, jnp.ones_like(v)], axis=1)


def weigh(scores, v):
    probs = [jnp.exp2((s - less) * LOG2E_SCALE).astype(jnp.bfloat16) for s, less in scores]
    return jnp.dot(jnp.concatenate(probs, axis=1), v, preferred_element_type=jnp.float32)


def attend_own(place, q_early, q_late, kv_early, kv_late, layout):
    heads = GROUP
    total = kv_early.shape[0] + kv_late.shape[0]
    rows = total // GROUP
    early = kv_early.shape[0]

    def kernel(place_ref, qe_ref, ql_ref, ke_ref, kl_ref, sums_ref, tops_ref, q_ref, s_ref):
        g, order = place_ref[1], pl.program_id(0)

        def sort():
            at = 0
            for j, first, n in layout:
                src = qe_ref[at : at + n] if at < early else ql_ref[at - early : at - early + n]
                q_ref[j * rows + first : j * rows + first + n] = src
                at += n

        pl.when(order == 0)(sort)
        at = pl.multiple_of(order * rows, rows)
        stacked = jnp.concatenate([q_ref[pl.ds(at, rows), h * HEAD : (h + 1) * HEAD] for h in range(heads)], axis=0)
        key_scores(s_ref, stacked, (ke_ref, kl_ref))
        v = values_and_ones((ke_ref, kl_ref))
        for h in range(heads):
            mine = slice(h * rows, (h + 1) * rows)
            scores, top, at = [], None, 0
            for j, first, n in layout:
                s = s_ref[mine, at : at + n]
                at += n
                ahead = lax.broadcasted_iota(jnp.int32, s.shape, 0) - lax.broadcasted_iota(jnp.int32, s.shape, 1)
                s = jnp.where(ahead >= ((g ^ j) - (g ^ order)) * rows + first, s, NEG)
                scores.append(s)
                top = best_of(s) if top is None else jnp.maximum(top, best_of(s))
            top = jnp.max(top, axis=1, keepdims=True)
            sums_ref[order, :, 2 * h * HEAD : 2 * (h + 1) * HEAD] = weigh([(s, top) for s in scores], v)
            tops_ref[order, :, h * HEAD : (h + 1) * HEAD] = jnp.broadcast_to(top, (rows, HEAD))

    vmem = pl.BlockSpec(memory_space=pltpu.VMEM)
    return pl.pallas_call(
        kernel,
        grid=(GROUP,),
        in_specs=[pl.BlockSpec(memory_space=pltpu.SMEM)] + [vmem] * 4,
        out_specs=[vmem] * 3,
        out_shape=[
            jax.ShapeDtypeStruct((GROUP, rows, 2 * heads * HEAD), jnp.float32),
            jax.ShapeDtypeStruct((GROUP, rows, heads * HEAD), jnp.float32),
            jax.ShapeDtypeStruct((total, heads * HEAD), jnp.bfloat16),
        ],
        scratch_shapes=[pltpu.VMEM((heads * rows, total), jnp.float32)],
        compiler_params=pltpu.CompilerParams(vmem_limit_bytes=16 << 20),
        cost_estimate=pl.CostEstimate(
            flops=8 * total * heads * HEAD * total, transcendentals=total * heads * total, bytes_accessed=3 << 20
        ),
    )(place, q_early, q_late, kv_early, kv_late)


def attend_below(place, sums, tops, queries, below, piece):
    heads = GROUP
    rows = queries.shape[0] // GROUP
    flat = [p for slab in below for p in slab]
    total = sum(p.shape[0] for p in flat)

    def kernel(place_ref, sums_ref, tops_ref, q_ref, *refs):
        kv = refs[: len(flat)]
        out_ref, s_ref = refs[len(flat) :]
        z = place_ref[0]

        def lowest():
            for h in range(heads):
                at = 2 * h * HEAD
                own = sums_ref[piece, :, at : at + 2 * HEAD]
                out_ref[:, h * HEAD : (h + 1) * HEAD] = (own[:, :HEAD] / own[:, HEAD:]).astype(jnp.bfloat16)

        def merged():
            first_row = piece * rows
            stacked = jnp.concatenate(
                [q_ref[first_row : first_row + rows, h * HEAD : (h + 1) * HEAD] for h in range(heads)], axis=0
            )
            key_scores(s_ref, stacked, kv)
            v = values_and_ones(kv)
            for h in range(heads):
                mine = slice(h * rows, (h + 1) * rows)
                old = tops_ref[piece, :, h * HEAD : (h + 1) * HEAD]
                found, top, at = [], old, 0
                for d, slab in enumerate(below, start=1):
                    n = sum(p.shape[0] for p in slab)
                    s = s_ref[mine, at : at + n]
                    at += n
                    found.append((s, z >= d))
                    top = jnp.maximum(top, jnp.where(z >= d, best_of(s), NEG))
                top = jnp.max(top, axis=1, keepdims=True)
                mixed = weigh([(s, jnp.where(visible, top, -NEG)) for s, visible in found], v)
                shrink = jnp.exp2((old - top) * LOG2E_SCALE)
                at = 2 * h * HEAD
                above = mixed[:, :HEAD] + sums_ref[piece, :, at : at + HEAD] * shrink
                under = mixed[:, HEAD:] + sums_ref[piece, :, at + HEAD : at + 2 * HEAD] * shrink
                out_ref[:, h * HEAD : (h + 1) * HEAD] = (above / under).astype(jnp.bfloat16)

        pl.when(z == 0)(lowest)
        pl.when(z > 0)(merged)

    vmem = pl.BlockSpec(memory_space=pltpu.VMEM)
    return pl.pallas_call(
        kernel,
        in_specs=[pl.BlockSpec(memory_space=pltpu.SMEM)] + [vmem] * (3 + len(flat)),
        out_specs=vmem,
        out_shape=jax.ShapeDtypeStruct((rows, heads * HEAD), jnp.bfloat16),
        scratch_shapes=[pltpu.VMEM((heads * rows, total), jnp.float32)],
        compiler_params=pltpu.CompilerParams(vmem_limit_bytes=28 << 20),
        cost_estimate=pl.CostEstimate(
            flops=8 * rows * heads * HEAD * total, transcendentals=rows * heads * total, bytes_accessed=3 << 20
        ),
    )(place, sums, tops, queries, *flat)


def section_tick(tokens, norm_gain, w_query, w_key, w_value):
    rank = lax.axis_index("seq")
    z, g = rank // GROUP, rank % GROUP
    place = jnp.stack([z, g]).astype(jnp.int32)
    rows = tokens.shape[1]
    half = rows // 2

    def columns(j):
        c = g ^ j
        take = lambda w, n: lax.dynamic_slice_in_dim(w[0], c * n, n, 1)
        return jnp.concatenate([take(w_query, 4 * HEAD), take(w_key, HEAD), take(w_value, HEAD)], axis=1)

    got = []
    for j in (1, 2, 3):
        got.append(near(columns(j), j))
    nq = GROUP * HEAD
    chip = jnp.concatenate([columns(0), got[0]], axis=0)
    other_kv = jnp.concatenate([got[1][:, nq:], got[2][:, nq:]], axis=0)
    other_q = jnp.concatenate([got[1][:, :nq], got[2][:, :nq]], axis=0)

    chip_left, chip_right = along(chip, 1), along(chip, -1)
    kv_left, kv_right = along(other_kv, 1), along(other_kv, -1)
    q_left, q_right = along(other_q, 1), along(other_q, -1)
    chip_far, kv_far, q_far = along(chip_left, 1), along(kv_right, -1), along(q_right, -1)
    offsets = (0, 1, 3, 2)
    kv_weights = [chip, other_kv, chip_right, kv_right, chip_left, kv_left, chip_far, kv_far]
    kv_bases = [nq, 0] * RING
    q_weights = [chip, other_q, chip_right, q_right, chip_left, q_left]

    normed, *halves = normalize(tokens[0], norm_gain)
    side = near(normed, 1)
    across, corner = [], []
    for i in range(2):
        across.append(near(halves[i], 2))
    for i in range(2):
        corner.append(near(across[i], 1))

    early = [(0, 0, rows), (1, 0, rows), (2, 0, half), (3, 0, half)]
    late = [(2, half, half), (3, half, half)]
    tables = rope_tables(z, g, rows, early + late)
    tokens_early = [normed, side, across[0], corner[0]]
    kv_early, kept_kv = project_kv(place, tokens_early, kv_weights, kv_bases, offsets, tables)
    raw, kept_q = project_most(place, tokens_early, q_weights, offsets[:3])
    q_early = project_rest(place, tokens_early, raw, [chip_far, q_far], offsets[3], tables)
    kv_late, q_late = project_late(place, [across[1], corner[1]], kept_kv, [kept_q, chip_far, q_far], offsets, tables)

    below = [[], [], []]
    for kv in (kv_early, kv_late):
        for d in (3, 2, 1):
            below[d - 1].append(upward(kv, [(z0, z0 + d) for z0 in range(RING - d)]))

    sums, tops, queries = attend_own(place, q_early, q_late, kv_early, kv_late, early + late)
    out = jnp.zeros((rows, GROUP * GROUP * HEAD), jnp.bfloat16)
    for k in (0, 1, 3, 2):
        mixed = attend_below(place, sums, tops, queries, below, k)
        arrived = onward(mixed, k)
        out = lax.dynamic_update_slice(out, arrived, (0, (g ^ k) * GROUP * HEAD))
    return out[None]


def solution(mesh):
    return jax.shard_map(
        section_tick,
        mesh=mesh,
        in_specs=(
            P("section", "seq", None),
            P("section", None),
            P("section", "seq", None),
            P("section", "seq", None),
            P("section", "seq", None),
        ),
        out_specs=P("section", "seq", None),
        check_vma=False,
    )
```
